32 devices in a mesh: comp: 2 (over core), dom: 16 (over z, y, x).
Axes of the slice: x: 2, y: 2, z: 4, core: 2. Of those that a mesh axis runs over, the one named last changes fastest.
Arguments:
- surface_flux: float32 [6, 12, 131072], P(None, None, ('comp', 'dom')), may hold values from -8 to 8
- active_mask: int32 [131072], P(('comp', 'dom')), may hold values 0 or 1
- source_area: float32 [131072], P(('comp', 'dom')), may hold values from 0.5 to 30
- tile_targets: int32 [2048, 2], P(('comp', 'dom')), may hold values from 0 to 31, all different within a row
- remap_tiles: float32 [2048, 2, 64, 384], P(('comp', 'dom')), may hold values from -0.0625 to 0.0625
- ocean_flux: float32 [12, 12288], P(None, ('comp', 'dom')), may hold values from -6 to 6
- air_fraction: float32 [3, 12288], P(None, ('comp', 'dom')), may hold values from 0 to 1, as said below
- air_area: float32 [12288], P(('comp', 'dom')), may hold values from 0.5 to 30
Outputs:
- merged: float32 [12, 12288], P(None, ('comp', 'dom'))
- area_means: float32 [3, 12], replicated
The draws below stay inside these ranges and needn't reach their ends.
Inputs may be any that keep to these rules, and one draw needn't show every extreme that they name: `air_fraction`: the three fractions of a cell are positive and sum to one. `tile_targets`: the 2 targets of one source block differ.
All inputs are finite; a program needn't handle non-finite values. No bound on the sum of `active_mask` on one device may be relied on, other than what follows from the above.
Results may differ from the reference program's by a relative error of at most 0.000071.
Values sent between devices are 32-bit elements; how exact they have to be, the bound alone decides.
No kernel may reach another device: no remote copies, remote signals or barrier semaphores. Data moves between devices by JAX's collectives and lax.ppermute only.
A program may use at most 64 MiB of HBM per device.

```python
import math
import jax
import jax.numpy as jnp
from jax import lax

FIELDS = 12
STEPS = 6
TOP = 2
BS = 64
SBLK = 64
ATM_DEV = 384
BLOCKS = 2048
SRC_CELLS = 131072
ATM_CELLS = 12288
N_COMP = 2
N_DOM = 16


def draw_surface_flux(key, part):
    subkeys = jax.random.split(key, 4)
    position = jnp.arange(SRC_CELLS, dtype=jnp.float32) / SRC_CELLS
    amplitude = jax.random.uniform(subkeys[0], (FIELDS, 1), jnp.float32, 0.5, 1.5)
    phase = jax.random.uniform(subkeys[1], (FIELDS, 1), jnp.float32, 0.0, 2.0 * math.pi)
    waves = 1.0 + (jnp.arange(FIELDS, dtype=jnp.int32) % 3).astype(jnp.float32)[:, None]
    offset = jax.random.uniform(subkeys[2], (FIELDS, 1), jnp.float32, -0.5, 0.5)
    trend = amplitude * jnp.cos(math.pi * waves * position[None, :] + phase) + offset
    noise = jax.random.normal(subkeys[3], (STEPS, FIELDS, SRC_CELLS), jnp.float32)
    return jnp.clip(trend[None, :, :] + noise, -8.0, 8.0)


def rising_area(key, total_cells):
    position = jnp.arange(total_cells, dtype=jnp.float32) / total_cells
    factor = jax.random.uniform(key, (total_cells,), jnp.float32, 0.5, 1.5)
    return (1.0 + 2.0 * position) * factor


def draw_source_area(key, part):
    return rising_area(jax.random.fold_in(key, 11), SRC_CELLS)


def draw_air_area(key, part):
    return rising_area(jax.random.fold_in(key, 23), ATM_CELLS)


def draw_air_fraction(key, part):
    shares = jax.random.uniform(key, (3, ATM_CELLS), jnp.float32, 0.1, 1.0)
    return shares / jnp.sum(shares, axis=0, keepdims=True)


def place_ends(result, key, smallest, largest):
    longest = result.shape.index(max(result.shape))
    spots = []
    for shift in (0, 1):
        where = [jax.random.randint(jax.random.fold_in(key, axis), (), 0, length) for axis, length in enumerate(result.shape)]
        where[longest] = (where[longest] + shift) % result.shape[longest]
        spots.append(tuple(where))
    return result.at[spots[0]].set(smallest).at[spots[1]].set(largest)


def shard_levels(own_key, shape, shards, smallest, largest):
    def one(axis_at, shards_of):
        heights = jax.random.uniform(jax.random.fold_in(jax.random.fold_in(own_key, 6), axis_at), (shards_of,), jnp.float32, smallest / len(shards), largest / len(shards))
        return jnp.repeat(jnp.exp(heights), shape[axis_at] // shards_of).reshape((-1,) + (1,) * (len(shape) - axis_at - 1))

    level = one(*shards[0])
    for cut in shards[1:]:
        level = level * one(*cut)
    return level


def different_ones(own_key, rows, number_of, top, lift):
    sequence = jax.random.permutation(jax.random.fold_in(own_key, 1), number_of)
    favour = sequence
    for power in range(3):
        favour = favour * favour // number_of
    favour = favour * lift // number_of
    lots = jax.random.randint(jax.random.fold_in(own_key, 2), (rows, number_of), 0, 4096) + favour
    holders = jax.random.permutation(jax.random.fold_in(own_key, 3), rows)[jnp.arange(number_of) % rows]
    lots = jnp.where(jnp.arange(rows)[:, None] == holders[None, :], 1 << 14, lots)
    priority = lots * number_of + jnp.arange(number_of)
    return lax.top_k(priority.astype(jnp.int32), top)[1].astype(jnp.int32)


def normal_values(rng, extent, spread, bound, cuts=(), kind=jnp.bfloat16):
    loudness = shard_levels(rng, extent, cuts, -0.22, 0.18) if cuts else 1.0
    result = jax.random.normal(rng, extent, jnp.float32) * spread * loudness
    return jnp.minimum(jnp.maximum(result, -bound), bound).astype(kind)


def setup_inputs(seed: int = 0) -> dict:
    streams_of = jax.random.split(jax.random.key(seed), 9)
    return {
        "surface_flux": draw_surface_flux(jax.random.fold_in(streams_of[8], 71), 0),
        "active_mask": place_ends((jax.random.randint(streams_of[1], (SRC_CELLS,), 0, 4) < 3).astype(jnp.int32), jax.random.fold_in(streams_of[1], 1), 0, 1),
        "source_area": draw_source_area(jax.random.fold_in(streams_of[8], 71), 0),
        "tile_targets": different_ones(streams_of[3], BLOCKS, N_COMP * N_DOM, TOP, 0),
        "remap_tiles": normal_values(streams_of[4], (BLOCKS, TOP, BS, ATM_DEV), (BS * SBLK * TOP) ** -0.5, 0.0625, ((0, 32),), jnp.float32),
        "ocean_flux": normal_values(streams_of[5], (FIELDS, ATM_CELLS), 1.0, 6.0, ((1, 32),), jnp.float32),
        "air_fraction": draw_air_fraction(jax.random.fold_in(streams_of[8], 71), 0),
        "air_area": draw_air_area(jax.random.fold_in(streams_of[8], 71), 0),
    }


def reference(surface_flux, active_mask, source_area, tile_targets, remap_tiles, ocean_flux, air_fraction, air_area):
    average = jnp.sum(surface_flux, axis=0) / STEPS
    weighted = average * (active_mask.astype(jnp.float32) * source_area)[None, :]
    blocks = weighted.reshape(FIELDS, BLOCKS, BS)
    contrib = jnp.einsum("fbs,btsa->btfa", blocks, remap_tiles, precision=lax.Precision.HIGHEST)
    contrib = contrib.reshape(BLOCKS * TOP, FIELDS, ATM_DEV)
    owner_total = N_COMP * N_DOM
    comp_of_block = (jnp.arange(BLOCKS, dtype=jnp.int32) // (SBLK * N_DOM)).astype(jnp.int32)
    segment = (comp_of_block[:, None] * owner_total + tile_targets).reshape(BLOCKS * TOP).astype(jnp.int32)
    summed = jax.ops.segment_sum(contrib, segment, num_segments=N_COMP * owner_total)
    summed = summed.reshape(N_COMP, owner_total, FIELDS, ATM_DEV).transpose(0, 2, 1, 3)
    remapped = summed.reshape(N_COMP, FIELDS, ATM_CELLS) / air_area[None, None, :]
    merged = air_fraction[0][None, :] * remapped[0] + air_fraction[1][None, :] * remapped[1] + air_fraction[2][None, :] * ocean_flux
    surface_num = jnp.sum(weighted.reshape(FIELDS, N_COMP, SRC_CELLS // N_COMP), axis=2).T
    surface_den = jnp.sum(source_area.reshape(N_COMP, SRC_CELLS // N_COMP), axis=1)
    air_num = jnp.sum(merged * air_area[None, :], axis=1)
    air_den = jnp.sum(air_area)
    area_means = jnp.concatenate([surface_num / surface_den[:, None], (air_num / air_den)[None, :]], axis=0)
    return merged, area_means
```

```python
import functools

import jax
import jax.numpy as jnp
from jax import lax
from jax.experimental import pallas as pl
from jax.experimental.pallas import tpu as pltpu
from jax.sharding import PartitionSpec as P

QUAD = 4
STEP_BLOCKS = 8
ROWS = 16


def split(x):
    hi = x.astype(jnp.bfloat16)
    lo = (x - hi.astype(jnp.float32)).astype(jnp.bfloat16)
    return hi, lo


def own_position():
    return lax.axis_index("comp") * lax.axis_size("dom") + lax.axis_index("dom")


def phase_plan(domain_count):
    plan, stride = [], 1
    while stride < domain_count:
        radix = 4 if domain_count // stride >= 4 else 2
        plan.append((radix, stride))
        stride *= radix
    return plan


def chunk_order(domain_count):
    order = [0]
    for radix, stride in reversed(phase_plan(domain_count)):
        order = [digit * stride + rest for digit in range(radix) for rest in order]
    return order


def remap_kernel(targets, flux, mask, area, tiles, sums, weighted_sum, padded):
    step = pl.program_id(0)
    me = own_position()
    step_count, field_count, _ = flux.shape
    block_cells = tiles.shape[2]
    air_cells = tiles.shape[3]
    cells = QUAD * block_cells
    lanes = mask.shape[1]

    @pl.when(step == 0)
    def _():
        sums[...] = jnp.zeros_like(sums)
        weighted_sum[...] = jnp.zeros_like(weighted_sum)
        padded[...] = jnp.zeros_like(padded)

    row_block = lax.broadcasted_iota(jnp.int32, (QUAD * ROWS, cells), 0) // ROWS
    col_block = lax.broadcasted_iota(jnp.int32, (QUAD * ROWS, cells), 1) // block_cells
    diagonal = row_block == col_block
    for quad in range(STEP_BLOCKS // QUAD):
        for part in range(cells // lanes):
            start = quad * cells + part * lanes
            row = step * (STEP_BLOCKS * block_cells // lanes) + start // lanes
            total = flux[0, :, start : start + lanes]
            for s in range(1, step_count):
                total = total + flux[s, :, start : start + lanes]
            coverage = mask[pl.ds(row, 1), :].astype(jnp.float32) * area[pl.ds(row, 1), :]
            weighted = (total / step_count) * coverage
            weighted_sum[0:field_count, :] += weighted
            padded[quad, 0:field_count, part * lanes : (part + 1) * lanes] = weighted
        value = padded[quad]
        left = jnp.where(diagonal, jnp.concatenate([value] * QUAD, axis=0), 0.0)
        left_hi, left_lo = split(left)
        left_both = jnp.concatenate([left_hi, left_lo], axis=0)
        for slot in range(tiles.shape[1]):
            right = tiles[quad * QUAD : (quad + 1) * QUAD, slot].reshape(cells, air_cells)
            right_hi, right_lo = split(right)
            first = jnp.dot(left_both, right_hi, preferred_element_type=jnp.float32)
            second = jnp.dot(left_hi, right_lo, preferred_element_type=jnp.float32)
            made = first[: QUAD * ROWS] + (first[QUAD * ROWS :] + second)
            for b in range(QUAD):
                target = targets[slot, step * STEP_BLOCKS + quad * QUAD + b]
                sums[target ^ me] += made[b * ROWS : (b + 1) * ROWS]


def as_row(column, width):
    eye = lax.broadcasted_iota(jnp.int32, (column.shape[0], width), 0) == lax.broadcasted_iota(
        jnp.int32, (column.shape[0], width), 1
    )
    return jnp.sum(jnp.where(eye, column, 0.0), axis=0, keepdims=True)


def weigh_kernel(order, sums, weighted_sum, shares, area, ocean, fraction, air_area, keep, send):
    me = own_position()
    own_group = lax.axis_index("comp")
    domain_count = len(order)
    field_count, width = ocean.shape
    total = jnp.zeros(sums.shape[1:], jnp.float32)
    for owner in range(2 * domain_count):
        total = total + sums[owner] * shares[owner ^ me]
    ocean_term = fraction[2:3, :] * ocean[...] * air_area[...]
    air_num = as_row(jnp.sum(total, axis=1, keepdims=True), width) + as_row(
        jnp.sum(ocean_term, axis=1, keepdims=True), width
    )
    air_den = jnp.sum(air_area[...])
    surface_num = as_row(jnp.sum(weighted_sum[...], axis=1, keepdims=True), width)
    surface_den = jnp.sum(area[...])
    lane = lax.broadcasted_iota(jnp.int32, (1, width), 1)
    surface = jnp.where(lane == field_count, surface_den, surface_num)
    air = jnp.where(lane == field_count, air_den, air_num)
    row = lax.broadcasted_iota(jnp.int32, (ROWS, width), 0)
    extra = jnp.where(row == field_count + own_group, surface, 0.0)
    extra = jnp.where(row == field_count + 2, air, extra)
    for slot, place in enumerate(order):
        keep[slot] = sums[place] * shares[place ^ me] + extra
        far = domain_count + place
        send[slot] = sums[far] * shares[far ^ me] + extra


def merge_kernel(*refs):
    pieces, (ocean, fraction, air_area, merged, means) = refs[:-5], refs[-5:]
    field_count = ocean.shape[0]
    total = tree_sum([piece[0] for piece in pieces])
    merged[...] = total[:field_count] / air_area[...] + fraction[2:3, :] * ocean[...]
    rows = total[field_count : field_count + 3]
    means[...] = rows[:, :field_count] / rows[:, field_count : field_count + 1]


def tree_sum(items):
    while len(items) > 1:
        items = [items[i] + items[i + 1] for i in range(0, len(items), 2)]
    return items[0]


def exchange(chunks, radix, stride):
    domain_count = lax.axis_size("dom")
    part = chunks.shape[0] // radix
    pieces = [chunks[:part]]
    for digit in range(1, radix):
        pairs = [(i, i ^ (digit * stride)) for i in range(domain_count)]
        pieces.append(lax.ppermute(chunks[digit * part : (digit + 1) * part], "dom", pairs))
    return pieces


def on_device(
    surface_flux,
    active_mask,
    source_area,
    tile_targets,
    remap_tiles,
    ocean_flux,
    air_fraction,
    air_area,
):
    step_count, field_count, cell_count = surface_flux.shape
    block_count, intersection, block_cells, air_cells = remap_tiles.shape
    group_count = lax.axis_size("comp")
    domain_count = lax.axis_size("dom")
    owner_count = group_count * domain_count
    lanes = 128
    order = chunk_order(domain_count)
    vmem = pl.BlockSpec(memory_space=pltpu.VMEM)

    mask = active_mask.reshape(cell_count // lanes, lanes)
    area = source_area.reshape(cell_count // lanes, lanes)
    air_row = air_area.reshape(1, air_cells)

    spread = jnp.broadcast_to(
        air_fraction[:group_count, None, None, :], (group_count, domain_count, 1, air_cells)
    ).reshape(owner_count, 1, air_cells)
    shares = lax.all_to_all(spread, ("comp", "dom"), split_axis=0, concat_axis=0, tiled=True)

    step_cells = STEP_BLOCKS * block_cells
    sums, weighted_sum = pl.pallas_call(
        remap_kernel,
        grid=(block_count // STEP_BLOCKS,),
        in_specs=[
            pl.BlockSpec(memory_space=pltpu.SMEM),
            pl.BlockSpec((step_count, field_count, step_cells), lambda i: (0, 0, i)),
            pl.BlockSpec((cell_count // lanes, lanes), lambda i: (0, 0)),
            pl.BlockSpec((cell_count // lanes, lanes), lambda i: (0, 0)),
            pl.BlockSpec((STEP_BLOCKS, intersection, block_cells, air_cells), lambda i: (i, 0, 0, 0)),
        ],
        out_specs=[
            pl.BlockSpec((owner_count, ROWS, air_cells), lambda i: (0, 0, 0)),
            pl.BlockSpec((ROWS, lanes), lambda i: (0, 0)),
        ],
        out_shape=[
            jax.ShapeDtypeStruct((owner_count, ROWS, air_cells), jnp.float32),
            jax.ShapeDtypeStruct((ROWS, lanes), jnp.float32),
        ],
        scratch_shapes=[
            pltpu.VMEM((STEP_BLOCKS // QUAD, ROWS, QUAD * block_cells), jnp.float32)
        ],
        cost_estimate=pl.CostEstimate(
            flops=2 * 16 * 6 * remap_tiles.size, bytes_accessed=4 * remap_tiles.size, transcendentals=0
        ),
        name="remap",
    )(tile_targets.T, surface_flux, mask, area, remap_tiles)

    half = jax.ShapeDtypeStruct((domain_count, ROWS, air_cells), jnp.float32)
    keep, send = pl.pallas_call(
        functools.partial(weigh_kernel, order),
        in_specs=[vmem] * 7,
        out_specs=[vmem] * 2,
        out_shape=[half, half],
        name="weigh",
    )(sums, weighted_sum, shares, area, ocean_flux, air_fraction, air_row)

    pairs = [(i, i ^ 1) for i in range(group_count)]
    chunks = keep + lax.ppermute(send, "comp", pairs)
    pieces = [chunks]
    for radix, stride in phase_plan(domain_count):
        pieces = exchange(tree_sum(pieces), radix, stride)

    merged, means = pl.pallas_call(
        merge_kernel,
        in_specs=[vmem] * (len(pieces) + 3),
        out_specs=[vmem] * 2,
        out_shape=[
            jax.ShapeDtypeStruct((field_count, air_cells), jnp.float32),
            jax.ShapeDtypeStruct((group_count + 1, field_count), jnp.float32),
        ],
        name="merge",
    )(*pieces, ocean_flux, air_fraction, air_row)
    return (merged, means)


def solution(mesh):
    in_specs = (
        P(None, None, ("comp", "dom")),
        P(("comp", "dom")),
        P(("comp", "dom")),
        P(("comp", "dom"), None),
        P(("comp", "dom"), None, None, None),
        P(None, ("comp", "dom")),
        P(None, ("comp", "dom")),
        P(("comp", "dom")),
    )
    out_specs = (P(None, ("comp", "dom")), P())
    return jax.shard_map(
        on_device, mesh=mesh, in_specs=in_specs, out_specs=out_specs, check_vma=False
    )
```

```python
import functools

import jax
import jax.numpy as jnp
from jax import lax
from jax.experimental import pallas as pl
from jax.experimental.pallas import tpu as pltpu
from jax.sharding import PartitionSpec as P

QUAD = 4
STEP_BLOCKS = 8
ROWS = 16


def split(x):
    hi = x.astype(jnp.bfloat16)
    lo = (x - hi.astype(jnp.float32)).astype(jnp.bfloat16)
    return hi, lo


def own_position():
    return lax.axis_index("comp") * lax.axis_size("dom") + lax.axis_index("dom")


def phase_plan(domain_count):
    plan, stride = [], 1
    while stride < domain_count:
        radix = 4 if domain_count // stride >= 4 else 2
        plan.append((radix, stride))
        stride *= radix
    return plan


def chunk_order(domain_count):
    order = [0]
    for radix, stride in reversed(phase_plan(domain_count)):
        order = [digit * stride + rest for digit in range(radix) for rest in order]
    return order


def remap_kernel(
    targets, flux_hbm, mask, area, tiles_hbm, sums, weighted_sum, flux, tiles, arrived, padded
):
    me = own_position()
    chunk_count, step_count, field_count, step_cells = flux.shape
    _, intersection, block_cells, air_cells = tiles_hbm.shape
    cells = QUAD * block_cells
    lanes = mask.shape[1]

    def copies(chunk):
        cell = chunk * step_cells
        block = chunk * STEP_BLOCKS
        return (
            pltpu.make_async_copy(
                flux_hbm.at[:, :, pl.ds(cell, step_cells)], flux.at[chunk], arrived.at[0, chunk]
            ),
            pltpu.make_async_copy(
                tiles_hbm.at[pl.ds(block, STEP_BLOCKS)],
                tiles.at[pl.ds(block, STEP_BLOCKS)],
                arrived.at[1, chunk],
            ),
        )

    for chunk in range(chunk_count):
        for copy in copies(chunk):
            copy.start()

    sums[...] = jnp.zeros_like(sums)
    weighted_sum[...] = jnp.zeros_like(weighted_sum)
    padded[...] = jnp.zeros_like(padded)
    row_block = lax.broadcasted_iota(jnp.int32, (QUAD * ROWS, cells), 0) // ROWS
    col_block = lax.broadcasted_iota(jnp.int32, (QUAD * ROWS, cells), 1) // block_cells
    diagonal = row_block == col_block

    @pl.loop(0, chunk_count)
    def _(chunk):
        for copy in copies(chunk):
            copy.wait()
        for quad in range(STEP_BLOCKS // QUAD):
            for part in range(cells // lanes):
                start = quad * cells + part * lanes
                row = chunk * (step_cells // lanes) + start // lanes
                total = flux[chunk, 0, :, start : start + lanes]
                for s in range(1, step_count):
                    total = total + flux[chunk, s, :, start : start + lanes]
                coverage = mask[pl.ds(row, 1), :].astype(jnp.float32) * area[pl.ds(row, 1), :]
                weighted = (total / step_count) * coverage
                weighted_sum[0:field_count, :] += weighted
                padded[quad, 0:field_count, part * lanes : (part + 1) * lanes] = weighted
            value = padded[quad]
            left = jnp.where(diagonal, jnp.concatenate([value] * QUAD, axis=0), 0.0)
            left_hi, left_lo = split(left)
            left_both = jnp.concatenate([left_hi, left_lo], axis=0)
            first_block = chunk * STEP_BLOCKS + quad * QUAD
            for slot in range(intersection):
                right = tiles[pl.ds(first_block, QUAD), slot].reshape(cells, air_cells)
                right_hi, right_lo = split(right)
                first = jnp.dot(left_both, right_hi, preferred_element_type=jnp.float32)
                second = jnp.dot(left_hi, right_lo, preferred_element_type=jnp.float32)
                made = first[: QUAD * ROWS] + (first[QUAD * ROWS :] + second)
                for b in range(QUAD):
                    sums[targets[slot, first_block + b] ^ me] += made[b * ROWS : (b + 1) * ROWS]


def as_row(column, width):
    eye = lax.broadcasted_iota(jnp.int32, (column.shape[0], width), 0) == lax.broadcasted_iota(
        jnp.int32, (column.shape[0], width), 1
    )
    return jnp.sum(jnp.where(eye, column, 0.0), axis=0, keepdims=True)


def weigh_kernel(order, sums, weighted_sum, shares, area, ocean, fraction, air_area, keep, send):
    me = own_position()
    own_group = lax.axis_index("comp")
    domain_count = len(order)
    field_count, width = ocean.shape
    air_row = air_area[...][None, :]
    total = jnp.zeros(sums.shape[1:], jnp.float32)
    for owner in range(2 * domain_count):
        total = total + sums[owner] * shares[owner ^ me]
    ocean_term = fraction[2:3, :] * ocean[...] * air_row
    air_num = as_row(jnp.sum(total, axis=1, keepdims=True), width) + as_row(
        jnp.sum(ocean_term, axis=1, keepdims=True), width
    )
    air_den = jnp.sum(air_row)
    surface_num = as_row(jnp.sum(weighted_sum[...], axis=1, keepdims=True), width)
    surface_den = jnp.sum(area[...])
    lane = lax.broadcasted_iota(jnp.int32, (1, width), 1)
    surface = jnp.where(lane == field_count, surface_den, surface_num)
    air = jnp.where(lane == field_count, air_den, air_num)
    row = lax.broadcasted_iota(jnp.int32, (ROWS, width), 0)
    extra = jnp.where(row == field_count + own_group, surface, 0.0)
    extra = jnp.where(row == field_count + 2, air, extra)
    for slot, place in enumerate(order):
        keep[slot] = sums[place] * shares[place ^ me] + extra
        far = domain_count + place
        send[slot] = sums[far] * shares[far ^ me] + extra


def tree_sum(items):
    while len(items) > 1:
        items = [items[i] + items[i + 1] for i in range(0, len(items), 2)]
    return items[0]


def cut(chunks, radix):
    part = chunks.shape[0] // radix
    return [chunks[digit * part : (digit + 1) * part] for digit in range(radix)]


def exchange(parts, stride):
    domain_count = lax.axis_size("dom")
    pieces = [parts[0]]
    for digit in range(1, len(parts)):
        pairs = [(i, i ^ (digit * stride)) for i in range(domain_count)]
        pieces.append(lax.ppermute(parts[digit], "dom", pairs))
    return pieces


def on_device(
    surface_flux,
    active_mask,
    source_area,
    tile_targets,
    remap_tiles,
    ocean_flux,
    air_fraction,
    air_area,
):
    step_count, field_count, cell_count = surface_flux.shape
    block_count, intersection, block_cells, air_cells = remap_tiles.shape
    group_count = lax.axis_size("comp")
    domain_count = lax.axis_size("dom")
    owner_count = group_count * domain_count
    lanes = 128
    order = chunk_order(domain_count)
    vmem = pl.BlockSpec(memory_space=pltpu.VMEM)

    mask = active_mask.reshape(cell_count // lanes, lanes)
    area = source_area.reshape(cell_count // lanes, lanes)

    spread = jnp.broadcast_to(
        air_fraction[:group_count, None, None, :], (group_count, domain_count, 1, air_cells)
    ).reshape(owner_count, 1, air_cells)
    shares = lax.all_to_all(spread, ("comp", "dom"), split_axis=0, concat_axis=0, tiled=True)

    step_cells = STEP_BLOCKS * block_cells
    chunk_count = block_count // STEP_BLOCKS
    half = jax.ShapeDtypeStruct((domain_count, ROWS, air_cells), jnp.float32)
    sums, weighted_sum = pl.pallas_call(
        remap_kernel,
        in_specs=[
            pl.BlockSpec(memory_space=pltpu.SMEM),
            pl.BlockSpec(memory_space=pl.ANY),
            vmem,
            vmem,
            pl.BlockSpec(memory_space=pl.ANY),
        ],
        out_specs=[vmem] * 2,
        out_shape=[
            jax.ShapeDtypeStruct((owner_count, ROWS, air_cells), jnp.float32),
            jax.ShapeDtypeStruct((ROWS, lanes), jnp.float32),
        ],
        scratch_shapes=[
            pltpu.VMEM((chunk_count, step_count, field_count, step_cells), jnp.float32),
            pltpu.VMEM(remap_tiles.shape, jnp.float32),
            pltpu.SemaphoreType.DMA((2, chunk_count)),
            pltpu.VMEM((STEP_BLOCKS // QUAD, ROWS, QUAD * block_cells), jnp.float32),
        ],
        cost_estimate=pl.CostEstimate(
            flops=2 * 16 * 6 * remap_tiles.size, bytes_accessed=4 * remap_tiles.size, transcendentals=0
        ),
        name="remap",
    )(tile_targets.T, surface_flux, mask, area, remap_tiles)

    keep, send = pl.pallas_call(
        functools.partial(weigh_kernel, order),
        in_specs=[vmem] * 7,
        out_specs=[vmem] * 2,
        out_shape=[half, half],
        name="weigh",
    )(sums, weighted_sum, shares, area, ocean_flux, air_fraction, air_area)

    pairs = [(i, i ^ 1) for i in range(group_count)]
    pieces = [keep, lax.ppermute(send, "comp", pairs)]
    for radix, stride in phase_plan(domain_count):
        pieces = exchange(cut(tree_sum(pieces), radix), stride)
    total = tree_sum(pieces)[0]
    merged = total[:field_count] / air_area[None, :] + air_fraction[2][None, :] * ocean_flux
    rows = total[field_count : field_count + group_count + 1]
    means = rows[:, :field_count] / rows[:, field_count : field_count + 1]
    return (merged, means)


def solution(mesh):
    in_specs = (
        P(None, None, ("comp", "dom")),
        P(("comp", "dom")),
        P(("comp", "dom")),
        P(("comp", "dom"), None),
        P(("comp", "dom"), None, None, None),
        P(None, ("comp", "dom")),
        P(None, ("comp", "dom")),
        P(("comp", "dom")),
    )
    out_specs = (P(None, ("comp", "dom")), P())
    return jax.shard_map(
        on_device, mesh=mesh, in_specs=in_specs, out_specs=out_specs, check_vma=False
    )
```
